32 devices in a mesh: row: 4 (over z), col: 8 (over y, x, core).
Axes of the slice: x: 2, y: 2, z: 4, core: 2. Of those that a mesh axis runs over, the one named last changes fastest.
Arguments:
- operator: bfloat16 [32768, 32768], P('row', 'col'), may hold values from -6 to 6
- right_test: bfloat16 [32768, 256], P('col'), may hold values from -0.03125 to 0.03125
- left_test: bfloat16 [32768, 384], P('row'), may hold values from -0.03125 to 0.03125
Outputs:
- left_factor: bfloat16 [32768, 256], P(('row', 'col'))
- right_factor: bfloat16 [32768, 256], P('col')
The draws below stay inside these ranges and needn't reach their ends.
All inputs are finite; a program needn't handle non-finite values.
Results may differ from the reference program's by a relative error of at most 0.0015.
Values may be sent and summed in bfloat16 or wider, within the bound.
A program may use at most 192 MiB of HBM per device.

```python
import jax
import jax.numpy as jnp
from jax import lax

N = 32768
R1 = 256
R2 = 384


def spiked(values, rng, source, target, blocks, factor):
    owner, partner = [(jnp.arange(values.shape[axis_at]) // (values.shape[axis_at] // blocks)).reshape([-1 if axis == axis_at else 1 for axis in range(values.ndim)]) for axis_at in (source, target)]
    chosen = jax.random.permutation(rng, blocks)[partner]
    strong = (owner == chosen) | (owner == (partner + blocks // 2) % blocks)
    return jnp.where(strong, factor * values, values)


def block_levels(own_key, extent, shards, low, largest):
    factor_of = 1.0
    for position, blocks in shards:
        draws = jax.random.uniform(jax.random.fold_in(jax.random.fold_in(own_key, 6), position), (blocks,), jnp.float32, low / len(shards), largest / len(shards))
        factor_of = factor_of * jnp.repeat(jnp.exp(draws), extent[position] // blocks).reshape((-1,) + (1,) * (len(extent) - 1 - position))
    return factor_of


def centred(stream_key, shape, width, reach, cuts=(), kind=jnp.bfloat16):
    level = block_levels(stream_key, shape, cuts, -0.22, 0.18) if cuts else 1.0
    drawn = jax.random.normal(stream_key, shape, jnp.float32) * width * level
    return jnp.minimum(jnp.maximum(drawn, -reach), reach).astype(kind)


def bell_draw_with(stream_key, extent, deviation, reach, cuts, heavy, held_as=jnp.bfloat16):
    result = deviation * jax.random.normal(stream_key, extent, jnp.float32)
    if cuts:
        result = result * block_levels(stream_key, extent, cuts, -0.22, 0.18)
    return jnp.clip(spiked(result, jax.random.fold_in(stream_key, 3), *heavy), -reach, reach).astype(held_as)


def setup_inputs(seed: int = 0) -> dict:
    seeds = jax.random.split(jax.random.key(seed), 4)
    operator = bell_draw_with(seeds[0], (N, N), 1.0, 6.0, ((0, 4), (1, 8)), (1, 0, 8, 2.0))
    right_test = centred(seeds[1], (N, R1), N ** -0.5, 0.03125, ((0, 8),))
    left_test = centred(seeds[2], (N, R2), N ** -0.5, 0.03125, ((0, 4),))
    return {"operator": operator, "right_test": right_test, "left_test": left_test}


def reference(operator, right_test, left_test):
    left_sketch = jnp.dot(operator.astype(jnp.float32), right_test.astype(jnp.float32), preferred_element_type=jnp.float32)
    right_sketch = lax.dot_general(operator.astype(jnp.float32), left_test.astype(jnp.float32), (((0,), (0,)), ((), ())), preferred_element_type=jnp.float32)
    core_matrix = lax.dot_general(left_test.astype(jnp.float32), left_sketch, (((0,), (0,)), ((), ())), precision=lax.Precision.HIGHEST)
    gram_plain = jnp.dot(core_matrix.T, core_matrix, precision=lax.Precision.HIGHEST)
    shift_size = 0.001 * jnp.trace(gram_plain) / R1
    gram_matrix = gram_plain + shift_size * jnp.eye(R1, dtype=jnp.float32)
    lower_factor = jnp.linalg.cholesky(gram_matrix)
    solve_map = jax.scipy.linalg.cho_solve((lower_factor, True), core_matrix.T)
    right_factor = jnp.dot(right_sketch, solve_map.T, precision=lax.Precision.HIGHEST).astype(jnp.bfloat16)
    return (left_sketch.astype(jnp.bfloat16), right_factor)
```

```python
import functools

import jax
import jax.numpy as jnp
from jax import lax
from jax.experimental import pallas as pl
from jax.experimental.pallas import tpu as pltpu
from jax.sharding import PartitionSpec as P

HIGHEST = lax.Precision.HIGHEST
F32 = jnp.float32
MESH = pl.DeviceIdType.MESH


def split3(x):
    a = x.astype(jnp.bfloat16)
    r = x - a.astype(F32)
    b = r.astype(jnp.bfloat16)
    c = (r - b.astype(F32)).astype(jnp.bfloat16)
    return a, b, c


def dot_rows(a, b, precision=None):
    return lax.dot_general(
        a, b, (((0,), (0,)), ((), ())), precision=precision, preferred_element_type=F32
    )


def bit_orders(count):
    bits = list(range(count.bit_length() - 1))
    return [bits, bits[:1] + bits[1:][::-1]]


def kernel(nr, nc, right_ref, left_ref, test_ref, left_out, right_out, *scratch):
    levels = nc.bit_length() - 1
    recv_left = scratch[:levels]
    (ring, core_own, core_col, core_row, core_all, work, solve_map,
     left_send, left_recv, ring_send, ring_recv, one_send, one_recv, two_send, two_recv,
     three_send, three_recv, ag_send, ag_recv) = scratch[levels:]
    row, col = lax.axis_index("row"), lax.axis_index("col")
    barrier = pltpu.get_barrier_semaphore()
    for i in range(1, nc):
        pl.semaphore_signal(barrier, inc=1, device_id={"col": lax.rem(col + i, nc)}, device_id_type=MESH)
    for i in range(1, nr):
        pl.semaphore_signal(barrier, inc=1, device_id={"row": lax.rem(row + i, nr)}, device_id_type=MESH)
    pl.semaphore_wait(barrier, nr + nc - 2)

    pending = []

    def send(src, dst, ssem, rsem, to):
        copy = pltpu.make_async_remote_copy(
            src_ref=src, dst_ref=dst, send_sem=ssem, recv_sem=rsem, device_id=to, device_id_type=MESH
        )
        copy.start()
        pending.append(copy)
        return copy

    chunk = right_ref.shape[0] // nr
    half = chunk // 2
    width = left_ref.shape[2]
    near = (lax.rem(row + 1, nr), lax.rem(row + nr - 1, nr))

    def rows_of(back, way):
        owner = lax.rem(row - back + 2 * nr, nr) if way == 0 else lax.rem(row + back, nr)
        return pl.ds(pl.multiple_of(owner * chunk + way * half, half), half)

    def ring_start(s):
        return [
            send(
                right_ref.at[rows_of(1, way)] if s == 0 else ring.at[way, s - 1],
                ring.at[way, s],
                ring_send.at[way, s],
                ring_recv.at[way, s],
                {"row": near[way]},
            )
            for way in range(2)
        ]

    def ring_add(s, copies):
        for way in range(2):
            copies[way].wait_recv()
            ring[way, s] += right_ref[rows_of(s + 2, way), :]

    orders = bit_orders(nc)
    lanes = width // 2

    def bit_of(b):
        return lax.rem(lax.div(col, 1 << b), 2)

    def left_index(order, level, e, flip):
        rest = order[level + 1:]
        total = jnp.int32(0)
        for b in order[: level + 1]:
            value = bit_of(b)
            if flip and b == order[level]:
                value = 1 - value
            total = total + value * (1 << b)
        for place, b in enumerate(rest):
            total = total + ((e >> place) & 1) * (1 << b)
        return total

    def left_source(h, level, e, flip):
        order = orders[h]
        if level == 0:
            return left_ref.at[left_index(order, 0, e, flip), :, pl.ds(h * lanes, lanes)]
        mine = bit_of(order[level])
        mine = 1 - mine if flip else mine
        return recv_left[level - 1].at[h, mine + 2 * e]

    def left_base(level):
        return sum(nc >> (l + 1) for l in range(level))

    def left_start(level):
        out = []
        for e in range(nc >> (level + 1)):
            for h in range(2):
                b = orders[h][level]
                partner = col + (1 - 2 * bit_of(b)) * (1 << b)
                at = left_base(level) + e
                out.append((h, e, send(
                    left_source(h, level, e, True),
                    recv_left[level].at[h, e],
                    left_send.at[h, at],
                    left_recv.at[h, at],
                    {"col": partner},
                )))
        return out

    def left_add(level, copies):
        for h, e, copy in copies:
            copy.wait_recv()
            recv_left[level][h, e] += left_source(h, level, e, False)[...]

    ring_now = ring_start(0)
    left_now = left_start(0)

    depth = left_ref.shape[1]

    core_own[...] = jnp.zeros_like(core_own)

    def core_step(c, carry):
        test = test_ref[pl.ds(pl.multiple_of(c * depth, depth), depth), :]
        a, b, d = split3(left_ref[c])
        core_own[...] += dot_rows(test, a) + (dot_rows(test, b) + dot_rows(test, d))
        return carry

    lax.fori_loop(0, nc, core_step, 0)

    piece = core_own.shape[0] // nc

    def piece_of(owner):
        return pl.ds(pl.multiple_of(owner * piece, piece), piece)

    one = []
    for i in range(1, nc):
        to = lax.rem(col + i, nc)
        one.append(send(core_own.at[piece_of(to)], core_col.at[i], one_send.at[i], one_recv.at[i], {"col": to}))
    for copy in one:
        copy.wait_recv()
    total = core_own[piece_of(col), :]
    for i in range(1, nc):
        total = total + core_col[i]
    core_row[0] = total
    two = []
    for i in range(1, nr):
        to = lax.rem(row + i, nr)
        two.append(send(core_row.at[0], core_row.at[i], two_send.at[i], two_recv.at[i], {"row": to}))
    left_add(0, left_now)
    ring_add(0, ring_now)
    if nr > 2:
        ring_now = ring_start(1)
    for copy in two:
        copy.wait_recv()
    for i in range(1, nr):
        total = total + core_row[i]
    core_all[piece_of(col), :] = total
    three = []
    for i in range(1, nc):
        to = lax.rem(col + i, nc)
        three.append(send(
            core_all.at[piece_of(col)], core_all.at[piece_of(col)], three_send.at[i], three_recv.at[i], {"col": to}
        ))
    left_now = left_start(1) if levels > 1 else None
    for copy in three:
        copy.wait_recv()

    core = core_all[...]
    gram = dot_rows(core, core, HIGHEST)
    ids = lax.broadcasted_iota(jnp.int32, (width, width), 0)
    cols = lax.broadcasted_iota(jnp.int32, (width, width), 1)
    shift = 0.001 * jnp.sum(jnp.where(ids == cols, gram, 0.0)) / width
    work[...] = gram + jnp.where(ids == cols, shift, 0.0)
    lane = lax.broadcasted_iota(jnp.int32, (1, width), 1)

    def step(k, carry):
        held = work[...]
        line = work[pl.ds(k, 1), :]
        at_k = cols == k
        column = jnp.sum(jnp.where(at_k, held, 0.0), axis=1, keepdims=True)
        pivot = 1.0 / jnp.sum(jnp.where(lane == k, line, 0.0), axis=1, keepdims=True)
        scaled = jnp.where(lane == k, pivot, line * pivot)
        work[...] = jnp.where(at_k, 0.0, held) - column * scaled
        work[pl.ds(k, 1), :] = scaled
        return carry

    jobs = []
    for s in range(1, nr - 1):
        jobs.append(("ring", s))
        if s < levels:
            jobs.append(("left", s))
    for level in range(nr - 1, levels):
        jobs.append(("left", level))
    if nr <= 2:
        jobs = [("left", level) for level in range(1, levels)]
    cut = len(jobs) + 1
    edges = [width * j // cut for j in range(cut + 1)]
    for j in range(cut):
        lax.fori_loop(edges[j], edges[j + 1], step, 0)
        if j < len(jobs):
            kind, s = jobs[j]
            if kind == "ring":
                ring_add(s, ring_now)
                if s < nr - 2:
                    ring_now = ring_start(s + 1)
            else:
                left_add(s, left_now)
                if s < levels - 1:
                    left_now = left_start(s + 1)
    solve_map[...] = jnp.dot(core, work[...], precision=HIGHEST, preferred_element_type=F32)

    def ag_start(s):
        out = []
        for way in range(2):
            part = right_out.at[rows_of(s, way)]
            out.append(send(part, part, ag_send.at[way, s], ag_recv.at[way, s], {"row": near[way]}))
        return out

    for way in range(2):
        right_out[rows_of(0, way), :] = jnp.dot(
            ring[way, nr - 2], solve_map[...], precision=HIGHEST, preferred_element_type=F32
        ).astype(jnp.bfloat16)
    ag_now = ag_start(0)
    for h in range(2):
        left_out[:, h * lanes:(h + 1) * lanes] = recv_left[levels - 1][h, 0].astype(jnp.bfloat16)
    for s in range(1, nr):
        for copy in ag_now:
            copy.wait_recv()
        if s < nr - 1:
            ag_now = ag_start(s)
    for copy in pending:
        copy.wait_send()


def exchange(nr, nc, right_block, left_block, left_test):
    rows, wide = right_block.shape
    depth, width = left_block.shape
    depth = depth // nc
    levels = nc.bit_length() - 1
    half = rows // nr // 2
    vmem = pl.BlockSpec(memory_space=pltpu.VMEM)
    dma = pltpu.SemaphoreType.DMA
    scratch = [pltpu.VMEM((2, nc >> (l + 1), depth, width // 2), F32) for l in range(levels)]
    scratch += [
        pltpu.VMEM((2, nr - 1, half, wide), F32),
        pltpu.VMEM((wide, width), F32),
        pltpu.VMEM((nc, wide // nc, width), F32),
        pltpu.VMEM((nr, wide // nc, width), F32),
        pltpu.VMEM((wide, width), F32),
        pltpu.VMEM((width, width), F32),
        pltpu.VMEM((wide, width), F32),
        dma((2, nc - 1)), dma((2, nc - 1)),
        dma((2, nr - 1)), dma((2, nr - 1)),
        dma((nc,)), dma((nc,)),
        dma((nr,)), dma((nr,)),
        dma((nc,)), dma((nc,)),
        dma((2, nr - 1)), dma((2, nr - 1)),
    ]
    return pl.pallas_call(
        functools.partial(kernel, nr, nc),
        out_shape=(
            jax.ShapeDtypeStruct((depth, width), jnp.bfloat16),
            jax.ShapeDtypeStruct((rows, width), jnp.bfloat16),
        ),
        in_specs=[vmem] * 3,
        out_specs=(vmem, vmem),
        scratch_shapes=scratch,
        compiler_params=pltpu.CompilerParams(
            collective_id=0, has_side_effects=True, vmem_limit_bytes=60 * 1024 * 1024
        ),
    )(right_block, left_block.reshape(nc, depth, width), left_test)


def body(nr, nc, operator, right_test, left_test):
    right_block = lax.dot_general(
        operator, left_test, (((0,), (0,)), ((), ())), preferred_element_type=F32
    )
    block_left = jnp.dot(operator, right_test, preferred_element_type=F32)
    return exchange(nr, nc, right_block, block_left, left_test)


def solution(mesh):
    placed = (P("row", "col"), P("col", None), P("row", None))
    return jax.shard_map(
        functools.partial(body, mesh.shape["row"], mesh.shape["col"]),
        mesh=mesh,
        in_specs=placed,
        out_specs=(P(("row", "col"), None), P("col", None)),
        check_vma=False,
    )
```
